128 devices in a mesh: data: 1, cp: 64 (over z, y, x), tp: 2 (over core).
Axes of the slice: x: 4, y: 4, z: 4, core: 2. Of those that a mesh axis runs over, the one named last changes fastest.
Arguments:
- act_in: bfloat16 [2, 8192, 2048], P(None, ('data', 'cp', 'tp'))
- route_ids: int32 [2, 8192, 2], P(None, ('data', 'cp', 'tp'))
- route_gates: float32 [2, 8192, 2], P(None, ('data', 'cp', 'tp'))
- w_query: bfloat16 [2048, 32, 128], P(None, 'tp')
- w_key: bfloat16 [2048, 4, 128], P(None, 'tp')
- w_value: bfloat16 [2048, 4, 128], P(None, 'tp')
- w_out: bfloat16 [32, 128, 2048], P('tp')
- w_gate: bfloat16 [128, 2048, 768], P(('cp', 'tp'))
- w_up: bfloat16 [128, 2048, 768], P(('cp', 'tp'))
- w_down: bfloat16 [128, 768, 2048], P(('cp', 'tp'))
Outputs:
- output: bfloat16 [2, 8192, 2048], P(None, ('data', 'cp', 'tp'))
All inputs are finite; a program needn't handle non-finite values.
Results may differ from the reference program's by a relative error of at most 0.00548.
Values are sent between devices in bfloat16 or wider.
A program may use at most 1 GiB of HBM per device.

```python
import math
import jax
import jax.numpy as jnp
from jax import lax

HIDDEN = 2048
EXPERT_FF = 768
Q_HEADS = 32
KV_HEADS = 4
HEAD_DIM = 128
CP_SIZE = 64
TP_SIZE = 2
TOKENS_DEV = 64
MICRO_BATCHES = 2

EXPERTS = CP_SIZE * TP_SIZE
SEQ_LEN = TOKENS_DEV * EXPERTS
PIECE_LEN = SEQ_LEN // (2 * CP_SIZE)
CAPACITY = (4 * TOKENS_DEV) // EXPERTS
EXPERT_ROWS = CAPACITY * EXPERTS
GROUP_SIZE = Q_HEADS // KV_HEADS
SCORE_SHARP = math.sqrt(0.75 * math.log(SEQ_LEN))


def draw_routing(base_key):
    half_cap = CAPACITY // 2

    def one_source(src_key):
        k_perm, k_delta, k_tok, k_swap = jax.random.split(src_key, 4)
        expert_perm = jax.random.permutation(k_perm, EXPERTS)
        deltas = jax.random.randint(k_delta, (EXPERTS // 2,), 0, half_cap + 1).at[0].set(half_cap)
        pair_counts = jnp.stack([half_cap + deltas, half_cap - deltas], axis=1).reshape(EXPERTS)
        counts = jnp.zeros((EXPERTS,), jnp.int32).at[expert_perm].set(pair_counts)
        count_ends = jnp.cumsum(counts)
        labels = jnp.sum((jnp.arange(2 * TOKENS_DEV)[:, None] >= count_ends[None, :]).astype(jnp.int32), axis=1)
        id_pairs = jnp.stack([labels[:TOKENS_DEV], labels[TOKENS_DEV:]], axis=1)
        id_pairs = id_pairs[jax.random.permutation(k_tok, TOKENS_DEV)]
        swap_flag = jax.random.randint(k_swap, (TOKENS_DEV, 1), 0, 2)
        return jnp.where(swap_flag == 1, id_pairs[:, ::-1], id_pairs).astype(jnp.int32)

    return jax.vmap(one_source)(jax.random.split(base_key, EXPERTS)).reshape(SEQ_LEN, 2)


def normal_weight(weight_key, arr_shape, w_scale):
    return (jax.random.normal(weight_key, arr_shape, jnp.float32) * w_scale).astype(jnp.bfloat16)


def expert_stack(weight_key, arr_shape, w_scale):
    return lax.map(lambda one_key: normal_weight(one_key, arr_shape, w_scale), jax.random.split(weight_key, EXPERTS))


def setup_inputs(seed: int = 0, part: int = 0) -> dict:
    part_key = jax.random.fold_in(jax.random.key(seed), part)
    k_act, k_route, k_gate = jax.random.split(part_key, 3)
    shared = jax.random.split(jax.random.key(seed + 1), 7)
    act_in = jax.random.normal(k_act, (MICRO_BATCHES, SEQ_LEN, HIDDEN), jnp.float32).astype(jnp.bfloat16)
    route_ids = jax.vmap(draw_routing)(jax.random.split(k_route, MICRO_BATCHES))
    route_gates = jax.random.uniform(k_gate, (MICRO_BATCHES, SEQ_LEN, 2), jnp.float32, 0.3, 0.7)
    return {
        'act_in': act_in,
        'route_ids': route_ids,
        'route_gates': route_gates,
        'w_query': normal_weight(shared[0], (HIDDEN, Q_HEADS, HEAD_DIM), SCORE_SHARP / math.sqrt(HIDDEN)),
        'w_key': normal_weight(shared[1], (HIDDEN, KV_HEADS, HEAD_DIM), 1.0 / math.sqrt(HIDDEN)),
        'w_value': normal_weight(shared[2], (HIDDEN, KV_HEADS, HEAD_DIM), 1.0 / math.sqrt(HIDDEN)),
        'w_out': normal_weight(shared[3], (Q_HEADS, HEAD_DIM, HIDDEN), 1.0 / math.sqrt(Q_HEADS * HEAD_DIM)),
        'w_gate': expert_stack(shared[4], (HIDDEN, EXPERT_FF), 1.0 / math.sqrt(HIDDEN)),
        'w_up': expert_stack(shared[5], (HIDDEN, EXPERT_FF), 1.0 / math.sqrt(HIDDEN)),
        'w_down': expert_stack(shared[6], (EXPERT_FF, HIDDEN), 1.0 / math.sqrt(EXPERT_FF)),
    }


def token_positions():
    row_ix = jnp.arange(SEQ_LEN)
    owner_ix = row_ix // (2 * PIECE_LEN)
    inner_ix = row_ix % (2 * PIECE_LEN)
    return jnp.where(inner_ix < PIECE_LEN, owner_ix * PIECE_LEN + inner_ix, (2 * CP_SIZE - 1 - owner_ix) * PIECE_LEN + inner_ix - PIECE_LEN)


def attention_block(seq_in, w_query, w_key, w_value, w_out):
    query_rows = jnp.dot(seq_in, w_query.reshape(HIDDEN, Q_HEADS * HEAD_DIM), preferred_element_type=jnp.float32).astype(jnp.bfloat16)
    key_rows = jnp.dot(seq_in, w_key.reshape(HIDDEN, KV_HEADS * HEAD_DIM), preferred_element_type=jnp.float32).astype(jnp.bfloat16)
    value_rows = jnp.dot(seq_in, w_value.reshape(HIDDEN, KV_HEADS * HEAD_DIM), preferred_element_type=jnp.float32).astype(jnp.bfloat16)
    key_rows = key_rows.astype(jnp.float32).reshape(SEQ_LEN, KV_HEADS, HEAD_DIM)
    value_rows = value_rows.astype(jnp.float32).reshape(SEQ_LEN, KV_HEADS, HEAD_DIM)
    positions = token_positions()
    query_blocks = query_rows.reshape(EXPERTS, TOKENS_DEV, KV_HEADS, GROUP_SIZE, HEAD_DIM)
    pos_blocks = positions.reshape(EXPERTS, TOKENS_DEV)

    def one_block(block_args):
        q_block, q_pos = block_args
        scores = jnp.einsum('qhgd,khd->hgqk', q_block.astype(jnp.float32), key_rows) * HEAD_DIM ** -0.5
        scores = jnp.where(positions[None, :] <= q_pos[:, None], scores, -jnp.inf)
        row_peak = jnp.max(scores, axis=-1, keepdims=True)
        exp_scores = jnp.exp(scores - row_peak)
        row_sum = jnp.sum(exp_scores, axis=-1)
        weighted = jnp.einsum('hgqk,khd->qhgd', exp_scores.astype(jnp.bfloat16).astype(jnp.float32), value_rows)
        weighted = weighted / jnp.transpose(row_sum, (2, 0, 1))[..., None]
        return weighted.astype(jnp.bfloat16).reshape(TOKENS_DEV, Q_HEADS * HEAD_DIM)

    attn_rows = lax.map(one_block, (query_blocks, pos_blocks)).reshape(SEQ_LEN, Q_HEADS * HEAD_DIM)
    attn_sum = jnp.dot(attn_rows, w_out.reshape(Q_HEADS * HEAD_DIM, HIDDEN), preferred_element_type=jnp.float32)
    return (seq_in.astype(jnp.float32) + attn_sum).astype(jnp.bfloat16)


def expert_block(mid_rows, seq_ids, seq_gates, w_gate, w_up, w_down):
    choice_expert = seq_ids.reshape(2 * SEQ_LEN)
    choice_token = jnp.arange(2 * SEQ_LEN) // 2
    sort_ix = jnp.argsort(choice_expert, stable=True)
    counts = jnp.sum((choice_expert[None, :] == jnp.arange(EXPERTS)[:, None]).astype(jnp.int32), axis=1)
    starts = jnp.cumsum(counts) - counts
    sorted_token = jnp.concatenate([choice_token[sort_ix], jnp.zeros((EXPERT_ROWS,), choice_token.dtype)])

    def one_expert(expert_id):
        token_ids = lax.dynamic_slice(sorted_token, (starts[expert_id],), (EXPERT_ROWS,))
        expert_in = mid_rows[token_ids]
        gate_act = jnp.dot(expert_in, w_gate[expert_id], preferred_element_type=jnp.float32)
        up_act = jnp.dot(expert_in, w_up[expert_id], preferred_element_type=jnp.float32)
        mixed_act = (jax.nn.silu(gate_act) * up_act).astype(jnp.bfloat16)
        return jnp.dot(mixed_act, w_down[expert_id], preferred_element_type=jnp.float32).astype(jnp.bfloat16)

    expert_out = lax.map(one_expert, jnp.arange(EXPERTS)).reshape(EXPERTS * EXPERT_ROWS, HIDDEN)
    sorted_expert = choice_expert[sort_ix]
    slot_rank = jnp.arange(2 * SEQ_LEN) - starts[sorted_expert]
    z_sorted = expert_out[sorted_expert * EXPERT_ROWS + slot_rank]
    z_choice = z_sorted[jnp.argsort(sort_ix)].reshape(SEQ_LEN, 2, HIDDEN)
    mixed_sum = jnp.sum(seq_gates[:, :, None] * z_choice.astype(jnp.float32), axis=1)
    return (mid_rows.astype(jnp.float32) + mixed_sum).astype(jnp.bfloat16)


def reference(act_in, route_ids, route_gates, w_query, w_key, w_value, w_out, w_gate, w_up, w_down):
    def one_sequence(seq_args):
        seq_in, seq_ids, seq_gates = seq_args
        mid_rows = attention_block(seq_in, w_query, w_key, w_value, w_out)
        return expert_block(mid_rows, seq_ids, seq_gates, w_gate, w_up, w_down)

    return lax.map(one_sequence, (act_in, route_ids, route_gates))
```

```python
import functools
import math

import jax
import jax.numpy as jnp
from jax import lax
from jax.experimental import pallas as pl
from jax.experimental.pallas import tpu as pltpu
from jax.sharding import PartitionSpec as P

F32 = jnp.float32
BF16 = jnp.bfloat16
HEAD = 128
GROUP = 8
PIECE = 64
TILE_PIECES = 8
TILE = TILE_PIECES * PIECE


def attn_kernel(cp_size, q_ref, k_ref, v_ref, o_ref, qs_ref, s_ref, mx_ref, l_ref, acc_ref):
    rank = lax.axis_index('cp')
    own_tile = rank // TILE_PIECES
    n_first = own_tile + 1
    half_tiles = cp_size // TILE_PIECES
    n_tiles = 2 * half_tiles + 1
    exp_scale = (HEAD ** -0.5) * math.log2(math.e)
    for piece in range(2):
        for g in range(GROUP):
            qs_ref[piece, g * PIECE:(g + 1) * PIECE, :] = q_ref[piece * PIECE:(piece + 1) * PIECE, g * HEAD:(g + 1) * HEAD]
    mx_ref[...] = jnp.full(mx_ref.shape, -jnp.inf, F32)
    l_ref[...] = jnp.zeros(l_ref.shape, F32)
    acc_ref[...] = jnp.zeros(acc_ref.shape, F32)
    row_in = lax.broadcasted_iota(jnp.int32, (TILE, 1), 0) % PIECE
    col = lax.broadcasted_iota(jnp.int32, (1, TILE), 1)

    def where_tile(i):
        is_first = i < n_first
        j = i - n_first
        lower = jnp.logical_or(is_first, j < half_tiles)
        half = jnp.where(lower, 0, 1)
        tile = jnp.where(is_first, i, jnp.where(lower, j, own_tile + j - half_tiles))
        return jnp.where(is_first, 0, 1), half, tile

    def key_slice(ref, half, tile):
        rows = ref[pl.ds(tile * TILE_PIECES, TILE_PIECES), pl.ds(pl.multiple_of(half * PIECE, PIECE), PIECE), :]
        return rows.reshape(TILE, HEAD)

    def score_step(i, carry):
        qi, half, tile = where_tile(i)
        s = lax.dot_general(qs_ref[qi], key_slice(k_ref, half, tile), (((1,), (1,)), ((), ())), preferred_element_type=F32)
        owner = tile * TILE_PIECES + col // PIECE
        key_piece = jnp.where(half == 0, owner, 2 * cp_size - 1 - owner)
        query_piece = jnp.where(qi == 0, rank, 2 * cp_size - 1 - rank)
        limit = (query_piece - key_piece) * PIECE - col % PIECE
        s = jnp.where(limit + row_in >= 0, s, -jnp.inf)
        s_ref[i] = s
        peak = mx_ref[qi]
        for b in range(TILE // HEAD):
            peak = jnp.maximum(peak, s[:, b * HEAD:(b + 1) * HEAD])
        mx_ref[qi] = peak
        return carry

    lax.fori_loop(0, n_tiles, score_step, 0)
    for piece in range(2):
        mx_ref[piece] = jnp.broadcast_to(jnp.max(mx_ref[piece], axis=1, keepdims=True), (TILE, HEAD))

    def value_step(i, carry):
        qi, half, tile = where_tile(i)
        peak = mx_ref[qi]
        total = l_ref[qi]
        blocks = []
        for b in range(TILE // HEAD):
            e = jnp.exp2((s_ref[i, :, b * HEAD:(b + 1) * HEAD] - peak) * exp_scale)
            total = total + e
            blocks.append(e.astype(BF16))
        l_ref[qi] = total
        e_tile = jnp.concatenate(blocks, axis=1)
        acc_ref[qi] += jnp.dot(e_tile, key_slice(v_ref, half, tile), preferred_element_type=F32)
        return carry

    lax.fori_loop(0, n_tiles, value_step, 0)
    for piece in range(2):
        out = (acc_ref[piece] / jnp.sum(l_ref[piece], axis=1, keepdims=True)).astype(BF16)
        for g in range(GROUP):
            o_ref[piece * PIECE:(piece + 1) * PIECE, g * HEAD:(g + 1) * HEAD] = out[g * PIECE:(g + 1) * PIECE, :]


def attention(q, kv, cp_size):
    kv3 = kv.reshape(cp_size, 2 * PIECE, kv.shape[-1])
    n_kv = kv.shape[-1] // HEAD // 2
    n_tiles = 2 * cp_size // TILE_PIECES + 1
    rows = 2 * PIECE
    return pl.pallas_call(
        functools.partial(attn_kernel, cp_size),
        out_shape=jax.ShapeDtypeStruct(q.shape, BF16),
        grid=(n_kv,),
        in_specs=[
            pl.BlockSpec((rows, GROUP * HEAD), lambda h: (0, h)),
            pl.BlockSpec((cp_size, rows, HEAD), lambda h: (0, 0, h)),
            pl.BlockSpec((cp_size, rows, HEAD), lambda h: (0, 0, n_kv + h)),
        ],
        out_specs=pl.BlockSpec((rows, GROUP * HEAD), lambda h: (0, h)),
        scratch_shapes=[
            pltpu.VMEM((2, TILE, HEAD), BF16),
            pltpu.VMEM((n_tiles, TILE, TILE), F32),
            pltpu.VMEM((2, TILE, HEAD), F32),
            pltpu.VMEM((2, TILE, HEAD), F32),
            pltpu.VMEM((2, TILE, HEAD), F32),
        ],
        compiler_params=pltpu.CompilerParams(vmem_limit_bytes=48 * 1024 * 1024),
        cost_estimate=pl.CostEstimate(flops=n_kv * n_tiles * TILE * TILE * HEAD * 4 * 2, bytes_accessed=kv.size * 2 + 2 * q.size * 2, transcendentals=n_kv * n_tiles * TILE * TILE),
        name='attention',
    )(q, kv3, kv3)


def solution(mesh):
    cp_size = mesh.shape['cp']
    tp_size = mesh.shape['tp']
    experts = cp_size * tp_size
    row_spec = P(None, ('data', 'cp', 'tp'), None)
    head_spec = P(None, 'tp', None)
    out_spec = P('tp', None, None)
    expert_spec = P(('cp', 'tp'), None, None)

    def device_step(act_in, route_ids, route_gates, w_query, w_key, w_value, w_out, w_gate, w_up, w_down):
        n_seq, tokens, hidden = act_in.shape
        x_half = lax.all_gather(act_in, 'tp', axis=1, tiled=True)
        kv_all = []
        for b in range(n_seq):
            k_half = jnp.einsum('sh,hnd->snd', x_half[b], w_key, preferred_element_type=F32).astype(BF16)
            v_half = jnp.einsum('sh,hnd->snd', x_half[b], w_value, preferred_element_type=F32).astype(BF16)
            kv = jnp.concatenate([k_half.reshape(2 * tokens, -1), v_half.reshape(2 * tokens, -1)], axis=1)
            kv_all.append(lax.all_gather(kv, 'cp', axis=0, tiled=True))
        q = jnp.einsum('bsh,hnd->bsnd', x_half, w_query, preferred_element_type=F32).astype(BF16)
        q = q.reshape(n_seq, 2 * tokens, -1)

        ids_chip = lax.all_gather(route_ids, 'tp', axis=0)
        flat = ids_chip.reshape(tp_size, n_seq, 2 * tokens)
        order = jnp.arange(2 * tokens)
        same = jnp.logical_and(flat[..., :, None] == flat[..., None, :], order[None, :] < order[:, None])
        slot = jnp.sum(same.astype(jnp.int32), axis=-1)
        part = (jnp.arange(tp_size)[:, None] * n_seq + jnp.arange(n_seq)[None, :])[..., None]
        row_of = (flat // tp_size) * (2 * tp_size * n_seq) + part * 2 + slot
        mine = flat % tp_size == lax.axis_index('tp')
        row_of = jnp.where(mine, row_of, -1).reshape(tp_size * n_seq * tokens, 2)
        slots = jnp.arange(cp_size * 2 * tp_size * n_seq, dtype=jnp.int32)
        pick0 = (row_of[:, 0:1] == slots[None, :])
        pick1 = (row_of[:, 1:2] == slots[None, :])
        send_pick = jnp.logical_or(pick0, pick1).astype(BF16)

        attn = [attention(q[b], kv_all[b], cp_size) for b in range(n_seq)]
        w_o = w_out.reshape(-1, hidden)
        partial = jnp.stack([jnp.dot(a, w_o, preferred_element_type=F32) for a in attn])
        attn_sum = lax.psum_scatter(partial, 'tp', scatter_dimension=1, tiled=True)
        h = (act_in.astype(F32) + attn_sum).astype(BF16)

        h_chip = lax.all_gather(h, 'tp', axis=0).reshape(tp_size * n_seq * tokens, hidden)
        send = lax.dot_general(send_pick, h_chip, (((0,), (0,)), ((), ())), preferred_element_type=F32).astype(BF16)
        recv = lax.all_to_all(send, 'cp', 0, 0, tiled=True)
        gate_act = jnp.dot(recv, w_gate[0], preferred_element_type=F32)
        up_act = jnp.dot(recv, w_up[0], preferred_element_type=F32)
        mixed = (jax.nn.silu(gate_act) * up_act).astype(BF16)
        z = jnp.dot(mixed, w_down[0], preferred_element_type=F32).astype(BF16)
        back = lax.all_to_all(z, 'cp', 0, 0, tiled=True)
        z0 = jnp.dot(pick0.astype(BF16), back, preferred_element_type=F32)
        z1 = jnp.dot(pick1.astype(BF16), back, preferred_element_type=F32)
        gates = lax.all_gather(route_gates, 'tp', axis=0).reshape(tp_size * n_seq * tokens, 2)
        mix = (gates[:, 0:1] * z0 + gates[:, 1:2] * z1).reshape(tp_size, n_seq, tokens, hidden)
        mix = lax.psum_scatter(mix, 'tp', scatter_dimension=0, tiled=False)
        return (h.astype(F32) + mix).astype(BF16)

    return jax.shard_map(device_step, mesh=mesh, in_specs=(row_spec, row_spec, row_spec, head_spec, head_spec, head_spec, out_spec, expert_spec, expert_spec, expert_spec), out_specs=row_spec, check_vma=False)
```
